32 devices in a mesh: band: 2 (over core), tmpl: 8 (over z, x), tm: 2 (over y).
Axes of the slice: x: 2, y: 2, z: 4, core: 2. Of those that a mesh axis runs over, the one named last changes fastest.
Arguments:
- strain_high: float32 [16384], P('tm'), may hold values from -6 to 6
- strain_mid: float32 [2048], P('tm'), may hold values from -6 to 6
- strain_low: float32 [256], P('tm'), may hold values from -6 to 6
- filters_high: float32 [320, 1024], P('tmpl'), may hold values from -0.1875 to 0.1875
- filters_mid: float32 [320, 1024], P('tmpl'), may hold values from -0.1875 to 0.1875
- filters_low: float32 [320, 128], P('tmpl'), may hold values from -0.5 to 0.5
- recon_high: float32 [320, 2, 2048], P(None, None, 'tmpl'), may hold values from -0.3125 to 0.3125
- recon_mid: float32 [320, 2, 2048], P(None, None, 'tmpl'), may hold values from -0.3125 to 0.3125
- recon_low: float32 [320, 2, 2048], P(None, None, 'tmpl'), may hold values from -0.3125 to 0.3125
- basis_count: int32 [3], replicated, may hold values from 160 to 320
Outputs:
- snr: float32 [2, 2048, 16384], P('band', 'tmpl', 'tm')
The draws below stay inside these ranges and needn't reach their ends.
Inputs may be any that keep to these rules, and one draw needn't show every extreme that they name: basis_count[b] says how many of the first 320 basis vectors band b uses.
All inputs are finite; a program needn't handle non-finite values.
Results may differ from the reference program's by a relative error of at most 0.000082.
Values sent between devices are 32-bit elements; how exact they have to be, the bound alone decides.
A program may use at most 128 MiB of HBM per device.

```python
import jax
import jax.numpy as jnp
from jax import lax

TEMPLATES = 2048
BASIS = 320
TAPS_HIGH = 1024
TAPS_MID = 1024
TAPS_LOW = 128
RATIO = 8
HALF_TAPS = 8
TIME = 16384
N_TMPL = 8


def block_scale(key, dims, cuts, smallest, largest):
    loudness = 1.0
    for dim, blocks in cuts:
        heights = jax.random.uniform(jax.random.fold_in(jax.random.fold_in(key, 6), dim), (blocks,), jnp.float32, smallest / len(cuts), largest / len(cuts))
        loudness = loudness * jnp.repeat(jnp.exp(heights), dims[dim] // blocks).reshape((-1,) + (1,) * (len(dims) - 1 - dim))
    return loudness


def centred(own_key, extent, deviation, limit, split=(), held_as=jnp.bfloat16):
    values = jax.random.normal(own_key, extent, jnp.float32) * deviation
    if len(split) > 0:
        values = block_scale(own_key, extent, split, -0.22, 0.18) * values
    return jnp.clip(values, min=-limit, max=limit).astype(held_as)


def setup_inputs(seed: int = 0) -> dict:
    keys = jax.random.split(jax.random.key(seed), 11)
    return {
        "strain_high": centred(keys[0], (TIME,), 1.0, 6.0, ((0, 2),), jnp.float32),
        "strain_mid": centred(keys[1], (TIME // RATIO,), 1.0, 6.0, ((0, 2),), jnp.float32),
        "strain_low": centred(keys[2], (TIME // (RATIO * RATIO),), 1.0, 6.0, ((0, 2),), jnp.float32),
        "filters_high": centred(keys[3], (BASIS, TAPS_HIGH), TAPS_HIGH ** -0.5, 0.1875, ((0, 8),), jnp.float32),
        "filters_mid": centred(keys[4], (BASIS, TAPS_MID), TAPS_MID ** -0.5, 0.1875, ((0, 8),), jnp.float32),
        "filters_low": centred(keys[5], (BASIS, TAPS_LOW), TAPS_LOW ** -0.5, 0.5, ((0, 8),), jnp.float32),
        "recon_high": centred(keys[6], (BASIS, 2, TEMPLATES), BASIS ** -0.5, 0.3125, ((2, 8),), jnp.float32),
        "recon_mid": centred(keys[7], (BASIS, 2, TEMPLATES), BASIS ** -0.5, 0.3125, ((2, 8),), jnp.float32),
        "recon_low": centred(keys[8], (BASIS, 2, TEMPLATES), BASIS ** -0.5, 0.3125, ((2, 8),), jnp.float32),
        "basis_count": jax.random.randint(keys[9], (3,), BASIS // 2, BASIS + 1).astype(jnp.int32),
    }


highest = lax.Precision.HIGHEST


def interp_value(offset, half_taps):
    return jnp.sinc(offset) * (0.5 + 0.5 * jnp.cos(jnp.pi * offset / (half_taps + 1)))


def interp_table(half_taps):
    phase_frac = jnp.arange(RATIO, dtype=jnp.float32)[:, None] / RATIO
    lag_index = jnp.arange(2 * half_taps, dtype=jnp.float32)[None, :]
    return interp_value(phase_frac - (lag_index - half_taps), half_taps)


def causal(series, filter_rows):
    tap_count = filter_rows.shape[1]
    padded = jnp.concatenate([jnp.zeros((tap_count - 1,), jnp.float32), series])
    result = lax.conv_general_dilated(padded[None, None, :], filter_rows[:, None, ::-1], (1,), "VALID", precision=highest)
    return result[0]


def masked(series, row_limit):
    row_index = jnp.arange(series.shape[0], dtype=jnp.int32)[:, None]
    return jnp.where(row_index < row_limit, series, 0.0)


def contract(weights, series):
    return lax.dot_general(weights, series, (((0,), (0,)), ((), ())), precision=highest, preferred_element_type=jnp.float32)


def upsample(signal, kernel_table):
    half_taps = kernel_table.shape[1] // 2
    channels, sample_count = signal.shape
    padded = jnp.pad(signal, ((0, 0), (half_taps, half_taps)))
    accumulated = jnp.zeros((channels, sample_count, RATIO), jnp.float32)
    for lag_index in range(2 * half_taps):
        accumulated = accumulated + padded[:, lag_index: lag_index + sample_count, None] * kernel_table[None, None, :, lag_index]
    return accumulated.reshape(channels, sample_count * RATIO)


def reference(strain_high, strain_mid, strain_low, filters_high, filters_mid, filters_low, recon_high, recon_mid, recon_low, basis_count):
    series_high = masked(causal(strain_high, filters_high), basis_count[0])
    series_mid = masked(causal(strain_mid, filters_mid), basis_count[1])
    series_low = masked(causal(strain_low, filters_low), basis_count[2])
    kernel_table = interp_table(HALF_TAPS)
    block_tmpl = TEMPLATES // N_TMPL
    starts = (jnp.arange(N_TMPL, dtype=jnp.int32) * block_tmpl).astype(jnp.int32)

    def one_block(start):
        def take_block(weights):
            return lax.dynamic_slice_in_dim(weights, start, block_tmpl, 2).reshape(BASIS, 2 * block_tmpl)

        low_snr = contract(take_block(recon_low), series_low)
        mid_snr = contract(take_block(recon_mid), series_mid) + upsample(low_snr, kernel_table)
        full_snr = contract(take_block(recon_high), series_high) + upsample(mid_snr, kernel_table)
        return full_snr.reshape(2, block_tmpl, TIME)

    blocks = lax.map(one_block, starts)
    return jnp.transpose(blocks, (1, 0, 2, 3)).reshape(2, TEMPLATES, TIME)
```

```python
import functools
import math

import jax
import jax.numpy as jnp
import numpy as np
from jax import lax
from jax.experimental import pallas as pl
from jax.experimental.pallas import tpu as pltpu
from jax.sharding import PartitionSpec as P

RATIO = 8
HALF_TAPS = 8
LANES = 128
WIDE = 256
MESH = pl.DeviceIdType.MESH


def upsample_matrix(rows, cols):
    u = np.arange(rows)[:, None]
    v = np.arange(cols)[None, :]
    lag = u - v // RATIO
    offset = (v % RATIO) / RATIO - (lag - HALF_TAPS)
    value = np.sinc(offset) * (0.5 + 0.5 * np.cos(np.pi * offset / (HALF_TAPS + 1)))
    return np.where((lag >= 0) & (lag < 2 * HALF_TAPS), value, 0.0).astype(np.float32)


def gather_kernel(
    sizes, low_ref, mid_ref, high_ref, strain_ref,
    low_all, mid_all, high_all, strain_all,
    send_sem, recv_sem, fsend_sem, frecv_sem, ssend_sem, srecv_sem,
):
    bands, peers, slices = sizes
    b, p, y = lax.axis_index("band"), lax.axis_index("tmpl"), lax.axis_index("tm")
    barrier = pltpu.get_barrier_semaphore()
    others = [(b, lax.rem(p + k, peers), y) for k in range(1, peers)]
    others += [(b, p, lax.rem(y + k, slices)) for k in range(1, slices)]
    others += [(1 - b, p, y)]
    for device in others:
        pl.semaphore_signal(barrier, inc=1, device_id=device, device_id_type=MESH)
    pl.semaphore_wait(barrier, len(others))

    strain_sends = []
    for k in range(1, slices):
        copy = pltpu.make_async_remote_copy(
            src_ref=strain_ref, dst_ref=strain_all.at[y],
            send_sem=ssend_sem.at[k], recv_sem=srecv_sem.at[k],
            device_id=(b, p, lax.rem(y + k, slices)), device_id_type=MESH,
        )
        copy.start()
        strain_sends.append(copy)

    mid_half = mid_ref.shape[1] // 2
    high_half = high_ref.shape[1] // 2
    mid_cols = pl.ds(pl.multiple_of(b * mid_half, LANES), mid_half)
    high_cols = pl.ds(pl.multiple_of(b * high_half, LANES), high_half)
    sends = {}
    for k in range(1, peers):
        target = (b, lax.rem(p + k, peers), y)
        pairs = (
            (low_ref, low_all.at[p]),
            (mid_ref.at[:, mid_cols], mid_all.at[p, :, mid_cols]),
            (high_ref.at[:, high_cols], high_all.at[p, :, high_cols]),
        )
        for a, (src, dst) in enumerate(pairs):
            copy = pltpu.make_async_remote_copy(
                src_ref=src, dst_ref=dst,
                send_sem=send_sem.at[a, k], recv_sem=recv_sem.at[a, k],
                device_id=target, device_id_type=MESH,
            )
            copy.start()
            sends[a, k] = copy
    low_all[p] = low_ref[...]
    mid_all[p] = mid_ref[...]
    high_all[p] = high_ref[...]
    strain_all[y] = strain_ref[...]

    forwards = []
    for k in range(1, peers):
        source = lax.rem(p + peers - k, peers)
        sends[0, k].wait_recv()
        for a, ref, cols in ((1, mid_all, mid_cols), (2, high_all, high_cols)):
            sends[a, k].wait_recv()
            view = ref.at[source, :, cols]
            copy = pltpu.make_async_remote_copy(
                src_ref=view, dst_ref=view,
                send_sem=fsend_sem.at[a - 1, k], recv_sem=frecv_sem.at[a - 1, k],
                device_id=(1 - b, p, y), device_id_type=MESH,
            )
            copy.start()
            forwards.append(copy)
    for copy in sends.values():
        copy.wait_send()
    for copy in strain_sends + forwards:
        copy.wait()


def gather(sizes, low, mid, high, strain):
    bands, peers, slices = sizes
    vmem = pl.BlockSpec(memory_space=pltpu.VMEM)
    shapes = [jax.ShapeDtypeStruct((peers,) + a.shape, a.dtype) for a in (low, mid, high)]
    shapes += [jax.ShapeDtypeStruct((slices,) + strain.shape, strain.dtype)]
    dma = pltpu.SemaphoreType.DMA
    return pl.pallas_call(
        functools.partial(gather_kernel, sizes),
        out_shape=shapes,
        in_specs=[vmem] * 4,
        out_specs=[vmem] * 4,
        scratch_shapes=[
            dma((3, peers)), dma((3, peers)), dma((2, peers)), dma((2, peers)),
            dma((slices,)), dma((slices,)),
        ],
        compiler_params=pltpu.CompilerParams(collective_id=0, has_side_effects=True),
        name="gather_filters",
    )(low, mid, high, strain)


def split(value):
    top = value.astype(jnp.bfloat16)
    return top, (value - top.astype(jnp.float32)).astype(jnp.bfloat16)


def dot3(a, b, dims=(((1,), (0,)), ((), ()))):
    def one(u, v):
        return lax.dot_general(u, v, dims, preferred_element_type=jnp.float32)

    return one(a[0], b[0]) + one(a[0], b[1]) + one(a[1], b[0])


def rolled(x_ref, row):
    base = jnp.broadcast_to(x_ref[pl.ds(row, 1), :], (LANES, LANES))
    return pltpu.roll(base, 0, 1, stride=1, stride_axis=0)


def fill_frames(x_ref, top_ref, rest_ref, chunks):
    lane = lax.broadcasted_iota(jnp.int32, (LANES, LANES), 1)
    lag = lax.broadcasted_iota(jnp.int32, (LANES, LANES), 0)

    def step(c, before):
        now = rolled(x_ref, c + 1)
        top, rest = split(jnp.where(lane >= lag, now, before))
        left = pl.multiple_of((chunks - 1 - c) * LANES, LANES)
        right = pl.multiple_of((chunks - c) * LANES, LANES)
        for ref, value in ((top_ref, top), (rest_ref, rest)):
            ref[pl.ds(left, LANES), :LANES] = value
            ref[pl.ds(right, LANES), LANES:] = value
        return now

    lax.fori_loop(0, chunks, step, rolled(x_ref, 0))


def compute_kernel(
    dims, clock_ref, low_f, mid_f, high_f, low_r, mid_r, high_r, x_low, x_mid, x_high, g_ref,
    out_ref,
    fl_top, fl_rest, fm_top, fm_rest, fh_top, fh_rest, w_top, w_rest, wm_top, wm_rest,
    p_top, p_rest, g_top, g_rest,
):
    low_here, mid_here, low_total, mid_total = dims
    step = pl.program_id(0)
    y = clock_ref[0]
    taps = high_f.shape[1]
    taps_mid = mid_f.shape[1]
    width = out_ref.shape[2]
    first = (((0,), (0,)), ((), ()))

    @pl.when(step == 0)
    def _():
        top, rest = split(g_ref[...])
        g_top[...] = top
        g_rest[...] = rest
        fill_frames(x_low, fl_top, fl_rest, x_low.shape[0] - 1)
        fill_frames(x_mid, fm_top, fm_rest, x_mid.shape[0] - 1)
        fill_frames(x_high, fh_top, fh_rest, x_high.shape[0] - 1)
        rows = lax.broadcasted_iota(jnp.int32, low_r.shape, 0)
        low_w = dot3(split(jnp.where(rows < clock_ref[3], low_r[...], 0.0)), split(low_f[...]), first)
        mid_w = dot3(split(jnp.where(rows < clock_ref[2], mid_r[...], 0.0)), split(mid_f[...]), first)
        high_w = dot3(split(jnp.where(rows < clock_ref[1], high_r[...], 0.0)), split(high_f[...]), first)
        wm_top[...], wm_rest[...] = split(mid_w)
        w_top[...], w_rest[...] = split(high_w)
        low_w = split(low_w)
        low_chunks = x_low.shape[0] - 1
        parts = []
        for c in range(low_chunks):
            at = (low_chunks - 1 - c) * LANES
            frames = (fl_top[at : at + LANES, :LANES], fl_rest[at : at + LANES, :LANES])
            parts.append(dot3(low_w, frames))
        low = jnp.concatenate(parts, axis=1)
        time = y * low_here - (HALF_TAPS + 1) + lax.broadcasted_iota(jnp.int32, low.shape, 1)
        low = split(jnp.where((time >= 0) & (time < low_total), low, 0.0))
        mid_chunks = x_mid.shape[0] - 1
        cols = p_top.shape[1]
        for start in range(0, cols, WIDE):
            size = min(WIDE, cols - start)
            at = (mid_chunks - taps_mid // LANES - start // LANES) * LANES
            frames = (fm_top[at : at + taps_mid, :size], fm_rest[at : at + taps_mid, :size])
            value = dot3((wm_top[...], wm_rest[...]), frames)
            base, lead = start // g_ref.shape[1] * LANES, start % g_ref.shape[1]
            pieces = tuple(v[:, base : base + WIDE] for v in low)
            value += dot3(pieces, (g_top[:, lead : lead + size], g_rest[:, lead : lead + size]))
            time = y * mid_here - HALF_TAPS + start + lax.broadcasted_iota(jnp.int32, value.shape, 1)
            top, rest = split(jnp.where((time >= 0) & (time < mid_total), value, 0.0))
            p_top[:, start : start + size] = top
            p_rest[:, start : start + size] = rest

    high_chunks = x_high.shape[0] - 1
    base = pl.multiple_of(step * (width // RATIO), LANES)
    pieces = (p_top[:, pl.ds(base, WIDE)], p_rest[:, pl.ds(base, WIDE)])
    for start in range(0, width, WIDE):
        at = (high_chunks - taps // LANES - start // LANES - step * (width // LANES)) * LANES
        rows = pl.ds(pl.multiple_of(at, LANES), taps)
        value = dot3((w_top[...], w_rest[...]), (fh_top[rows, :], fh_rest[rows, :]))
        tile = slice(start, start + WIDE)
        out_ref[0, :, tile] = value + dot3(pieces, (g_top[:, tile], g_rest[:, tile]))


def compute(dims, clock, filters, recons, strains):
    low_here, mid_here, low_total, mid_total = dims
    tmpl = recons[0].shape[1]
    x_low, x_mid, x_high = strains
    taps = filters[2].shape[1]
    samples = x_high.shape[0] * LANES - taps
    width = RATIO * LANES
    cols = mid_here + LANES
    g = jnp.asarray(upsample_matrix(WIDE, width))
    half = jnp.bfloat16

    def frames(x):
        return [pltpu.VMEM((x.shape[0] * LANES, WIDE), half)] * 2

    full = [pl.BlockSpec(memory_space=pltpu.VMEM)] * 10
    return pl.pallas_call(
        functools.partial(compute_kernel, dims),
        grid=(samples // width,),
        out_shape=jax.ShapeDtypeStruct((1, tmpl, samples), jnp.float32),
        in_specs=[pl.BlockSpec(memory_space=pltpu.SMEM)] + full,
        out_specs=pl.BlockSpec((1, tmpl, width), lambda i: (0, 0, i)),
        scratch_shapes=frames(x_low) + frames(x_mid) + frames(x_high)
        + [pltpu.VMEM((tmpl, taps), half)] * 2
        + [pltpu.VMEM((tmpl, filters[1].shape[1]), half)] * 2
        + [pltpu.VMEM((tmpl, cols), half)] * 2
        + [pltpu.VMEM((WIDE, width), half)] * 2,
        compiler_params=pltpu.CompilerParams(vmem_limit_bytes=60 * 1024 * 1024),
        name="filter_templates",
    )(clock, *filters, *recons, x_low, x_mid, x_high, g)


def local(
    sizes, strain_high, strain_mid, strain_low, filters_high, filters_mid, filters_low,
    recon_high, recon_mid, recon_low, basis_count,
):
    bands, peers, slices = sizes
    b, y = lax.axis_index("band"), lax.axis_index("tm")
    n_high, n_mid, n_low = strain_high.shape[0], strain_mid.shape[0], strain_low.shape[0]
    packed = jnp.concatenate([strain_high, strain_mid, strain_low]).reshape(-1, LANES)
    low, mid, high, strains = gather(sizes, filters_low, filters_mid, filters_high, packed)
    strains = strains.reshape(slices, -1)

    def window(start, count, before, rows):
        whole = strains[:, start : start + count].reshape(-1)
        whole = jnp.pad(whole, (before, rows * LANES))
        return lax.dynamic_slice(whole, (y * count,), (rows * LANES,)).reshape(rows, LANES)

    taps_high, taps_mid, taps_low = (f.shape[1] for f in (filters_high, filters_mid, filters_low))
    x_high = window(0, n_high, taps_high, (n_high + taps_high) // LANES)
    x_mid = window(n_high, n_mid, taps_mid + HALF_TAPS, (n_mid + LANES + taps_mid) // LANES)
    x_low = window(n_high + n_mid, n_low, taps_low + HALF_TAPS + 1, (n_low + 2 * LANES + taps_low) // LANES)

    def part(recon):
        return lax.dynamic_index_in_dim(recon, b, 1, keepdims=False)

    def flat(f):
        return f.reshape(-1, f.shape[2])

    clock = jnp.concatenate([y[None].astype(jnp.int32), basis_count])
    return compute(
        (n_low, n_mid, n_low * slices, n_mid * slices), clock,
        (flat(low), flat(mid), flat(high)),
        (part(recon_low), part(recon_mid), part(recon_high)),
        (x_low, x_mid, x_high),
    )


def solution(mesh):
    sizes = tuple(mesh.shape[name] for name in ("band", "tmpl", "tm"))
    in_specs = (
        P("tm"), P("tm"), P("tm"),
        P("tmpl", None), P("tmpl", None), P("tmpl", None),
        P(None, None, "tmpl"), P(None, None, "tmpl"), P(None, None, "tmpl"),
        P(),
    )
    return jax.shard_map(
        functools.partial(local, sizes), mesh=mesh, in_specs=in_specs,
        out_specs=P("band", "tmpl", "tm"), check_vma=False,
    )
```

```python
import functools
import math

import jax
import jax.numpy as jnp
import numpy as np
from jax import lax
from jax.experimental import pallas as pl
from jax.experimental.pallas import tpu as pltpu
from jax.sharding import PartitionSpec as P

RATIO = 8
HALF_TAPS = 8
LANES = 128
WIDE = 256
MESH = pl.DeviceIdType.MESH


def upsample_matrix(rows, cols):
    u = np.arange(rows)[:, None]
    v = np.arange(cols)[None, :]
    lag = u - v // RATIO
    offset = (v % RATIO) / RATIO - (lag - HALF_TAPS)
    value = np.sinc(offset) * (0.5 + 0.5 * np.cos(np.pi * offset / (HALF_TAPS + 1)))
    return np.where((lag >= 0) & (lag < 2 * HALF_TAPS), value, 0.0).astype(np.float32)


def gather_kernel(
    sizes, low_ref, mid_ref, high_ref, sl_ref, sm_ref, sh_ref,
    low_all, mid_all, high_all, sl_all, sm_all, sh_prev,
    strain_send, strain_recv, lz_send, lz_recv, lx_send, lx_recv,
    z_send, z_recv, x_send, x_recv, y_send, y_recv, d_send, d_recv, c_send, c_recv,
):
    bands, peers, slices, lines, parts = sizes
    rings = peers // lines
    b, p, y = lax.axis_index("band"), lax.axis_index("tmpl"), lax.axis_index("tm")
    z, x = p // lines, p % lines
    part = y % parts

    def along_z(k):
        return (b, ((z + k) % rings) * lines + x, y)

    def along_y(m):
        return (b, p, y - part + (part + m) % parts)

    across = (b, z * lines + (x + 1) % lines, y)
    sibling = (1 - b, p, y)
    barrier = pltpu.get_barrier_semaphore()
    others = [along_z(k) for k in range(1, rings)] + [sibling]
    others += [(b, p, (y + k) % slices) for k in range(1, slices)]
    if lines > 1:
        others += [across]
    for device in others:
        pl.semaphore_signal(barrier, inc=1, device_id=device, device_id_type=MESH)
    pl.semaphore_wait(barrier, len(others))

    sent, landed = [], []

    def send(src, dst, sems, at, device):
        copy = pltpu.make_async_remote_copy(
            src_ref=src, dst_ref=dst, send_sem=sems[0].at[at], recv_sem=sems[1].at[at],
            device_id=device, device_id_type=MESH,
        )
        copy.start()
        sent.append(copy)
        return copy

    strain = (strain_send, strain_recv)
    for k in range(1, slices):
        device = (b, p, (y + k) % slices)
        landed.append(send(sl_ref, sl_all.at[2 + y], strain, (0, k), device))
        landed.append(send(sm_ref, sm_all.at[2 + y], strain, (1, k), device))
    if slices > 1:
        tail = sh_prev.shape[0]
        last = sh_ref.at[pl.ds(sh_ref.shape[0] - tail, tail)]
        landed.append(send(last, sh_prev, strain, (2, 1), (b, p, (y + 1) % slices)))

    arrays = ((mid_ref, mid_all), (high_ref, high_all))
    size = [ref.shape[1] // (bands * parts) for ref, _ in arrays]

    def cols(a, m=0):
        start = (b * parts + (part + m) % parts) * size[a]
        return pl.ds(pl.multiple_of(start, LANES), size[a])

    def shard(k, other=0):
        return ((z + rings - k) % rings) * lines + (x + other) % lines

    low_z = {k: send(low_ref, low_all.at[p], (lz_send, lz_recv), k, along_z(k)) for k in range(1, rings)}
    from_z, from_x, from_y, from_d = {}, {}, {}, {}
    low_x = {}
    if lines > 1:
        low_x[0] = send(low_ref, low_all.at[p], (lx_send, lx_recv), 0, across)
    for a, (ref, full) in enumerate(arrays):
        for k in range(1, rings):
            from_z[a, k] = send(
                ref.at[:, cols(a)], full.at[p, :, cols(a)], (z_send, z_recv), (a, k), along_z(k)
            )
        if lines > 1:
            for m in range(parts):
                piece = send(
                    ref.at[:, cols(a, m)], full.at[p, :, cols(a, m)],
                    (x_send, x_recv) if m == 0 else (d_send, d_recv), (a, m, 0), across,
                )
                (from_x if m == 0 else from_d)[a, m, 0] = piece
    low_all[p] = low_ref[...]
    mid_all[p] = mid_ref[...]
    high_all[p] = high_ref[...]
    for ref, value in ((sl_all, sl_ref), (sm_all, sm_ref)):
        zero = jnp.zeros(value.shape, jnp.float32)
        ref[0] = zero
        ref[1] = zero
        ref[slices + 2] = zero
        ref[slices + 3] = zero
        ref[2 + y] = value[...]
    if slices == 1:
        sh_prev[...] = jnp.zeros(sh_prev.shape, jnp.float32)

    count = [0]

    def pass_on(a, view):
        at = (a, count[0])
        count[0] += 1
        landed.append(send(view, view, (c_send, c_recv), at, sibling))

    for k in range(1, rings):
        low_z[k].wait_recv()
        if lines > 1:
            view = low_all.at[shard(k)]
            low_x[k] = send(view, view, (lx_send, lx_recv), k, across)
    for a, (_, full) in enumerate(arrays):
        count[0] = 0
        for k in range(1, rings):
            from_z[a, k].wait_recv()
            view = full.at[shard(k), :, cols(a)]
            if lines > 1:
                from_x[a, 0, k] = send(view, view, (x_send, x_recv), (a, 0, k), across)
            for m in range(1, parts):
                from_y[a, m, k] = send(view, view, (y_send, y_recv), (a, m, k), along_y(m))
            pass_on(a, view)
    base = count[0]
    for a, (_, full) in enumerate(arrays):
        count[0] = base
        for k in range(rings):
            if lines > 1:
                from_x[a, 0, k].wait_recv()
                view = full.at[shard(k, 1), :, cols(a)]
                if k % 2 == 1:
                    for m in range(1, parts):
                        from_d[a, m, k] = send(view, view, (d_send, d_recv), (a, m, k), along_y(m))
                pass_on(a, view)
            for m in range(1, parts):
                if k == 0:
                    continue
                from_y[a, m, k].wait_recv()
                view = full.at[shard(k), :, cols(a, parts - m)]
                if lines > 1 and k % 2 == 0:
                    from_d[a, m, k] = send(view, view, (d_send, d_recv), (a, m, k), across)
                pass_on(a, view)
    base = count[0]
    for a, (_, full) in enumerate(arrays):
        count[0] = base
        for k in range(rings):
            for m in range(1, parts):
                if lines > 1:
                    from_d[a, m, k].wait_recv()
                    shift = m if k == 0 else parts - m
                    pass_on(a, full.at[shard(k, 1), :, cols(a, shift)])
    for copy in low_x.values():
        copy.wait_recv()
    for copy in landed:
        copy.wait_recv()
    for copy in sent:
        copy.wait_send()


def gather(sizes, low, mid, high, s_low, s_mid, s_high):
    bands, peers, slices = sizes
    lines = 2 if peers % 2 == 0 else 1
    rings = peers // lines
    parts = math.gcd(slices, min(mid.shape[1], high.shape[1]) // (bands * LANES))
    vmem = pl.BlockSpec(memory_space=pltpu.VMEM)
    f32 = jnp.float32
    shapes = [jax.ShapeDtypeStruct((peers,) + a.shape, f32) for a in (low, mid, high)]
    shapes += [jax.ShapeDtypeStruct((slices + 4,) + a.shape, f32) for a in (s_low, s_mid)]
    shapes += [jax.ShapeDtypeStruct((high.shape[1] // LANES, LANES), f32)]
    dma = pltpu.SemaphoreType.DMA
    two = lambda *dims: [dma(dims)] * 2
    return pl.pallas_call(
        functools.partial(gather_kernel, (bands, peers, slices, lines, parts)),
        out_shape=shapes,
        in_specs=[vmem] * 6,
        out_specs=[vmem] * 6,
        scratch_shapes=two(3, slices) + two(rings) + two(rings) + two(2, rings)
        + two(2, parts, rings) * 3 + two(2, peers * parts),
        compiler_params=pltpu.CompilerParams(collective_id=0, has_side_effects=True),
        name="gather_filters",
    )(low, mid, high, s_low, s_mid, s_high)


def split(value):
    top = value.astype(jnp.bfloat16)
    return top, (value - top.astype(jnp.float32)).astype(jnp.bfloat16)


def dot3(a, b, dims=(((1,), (0,)), ((), ()))):
    def one(u, v):
        return lax.dot_general(u, v, dims, preferred_element_type=jnp.float32)

    return one(a[0], b[0]) + one(a[0], b[1]) + one(a[1], b[0])


def staggered(row):
    return pltpu.roll(jnp.broadcast_to(row, (LANES, LANES)), 0, 1, stride=1, stride_axis=0)


def shifted(read, by):
    lane = lax.broadcasted_iota(jnp.int32, (1, LANES), 1)

    def row(r):
        late = [pltpu.roll(read(r + i), by, 1) for i in range(2)]
        return jnp.where(lane >= by, late[1], late[0])

    return row


def fill_frames(row, top_ref, rest_ref, chunks):
    lane = lax.broadcasted_iota(jnp.int32, (LANES, LANES), 1)
    lag = lax.broadcasted_iota(jnp.int32, (LANES, LANES), 0)

    def step(c, before):
        now = staggered(row(c + 1))
        top, rest = split(jnp.where(lane >= lag, now, before))
        left = pl.multiple_of((chunks - 1 - c) * LANES, LANES)
        right = pl.multiple_of((chunks - c) * LANES, LANES)
        for ref, value in ((top_ref, top), (rest_ref, rest)):
            ref[pl.ds(left, LANES), :LANES] = value
            ref[pl.ds(right, LANES), LANES:] = value
        return now

    lax.fori_loop(0, chunks, step, staggered(row(0)))


def compute_kernel(
    dims, count_ref, low_f, mid_f, high_f, x_low, x_mid, x_prev, x_high, g_ref,
    recon_low, recon_mid, recon_high,
    out_ref, low_r, mid_r, high_r, recon_sem, x_full,
    fl_top, fl_rest, fm_top, fm_rest, fh_top, fh_rest, w_top, w_rest, wm_top, wm_rest,
    p_top, p_rest, g_top, g_rest,
):
    low_here, mid_here, low_total, mid_total = dims
    step = pl.program_id(0)
    y = lax.axis_index("tm")
    taps = high_f.shape[1]
    taps_mid = mid_f.shape[1]
    taps_low = low_f.shape[1]
    low_chunks, mid_chunks, high_chunks = (r.shape[0] // LANES - 1 for r in (fl_top, fm_top, fh_top))
    width = out_ref.shape[2]
    first = (((0,), (0,)), ((), ()))

    @pl.when(step == 0)
    def _():
        top, rest = split(g_ref[...])
        g_top[...] = top
        g_rest[...] = rest
        band = lax.axis_index("band")
        copies = []
        for i, (src, dst) in enumerate(((recon_low, low_r), (recon_mid, mid_r), (recon_high, high_r))):
            copy = pltpu.make_async_copy(src.at[:, band, :], dst, recon_sem.at[i])
            copy.start()
            copies.append(copy)
        before = x_prev.shape[0]
        x_full[:before] = jnp.where(y > 0, x_prev[...], 0.0)
        x_full[before:] = x_high[...]
        low_first = y + 2 - taps_low // LANES - 1
        mid_first = (y + 2) * (mid_here // LANES) - taps_mid // LANES - 1
        low_row = shifted(lambda r: x_low[low_first + r], HALF_TAPS + 1)
        mid_row = shifted(lambda r: x_mid[pl.ds(mid_first + r, 1), :], HALF_TAPS)
        fill_frames(low_row, fl_top, fl_rest, low_chunks)
        fill_frames(mid_row, fm_top, fm_rest, mid_chunks)
        fill_frames(lambda r: x_full[pl.ds(r, 1), :], fh_top, fh_rest, high_chunks)
        for copy in copies:
            copy.wait()
        rows = lax.broadcasted_iota(jnp.int32, low_r.shape, 0)
        low_w = dot3(split(jnp.where(rows < count_ref[2], low_r[...], 0.0)), split(low_f[...]), first)
        mid_w = dot3(split(jnp.where(rows < count_ref[1], mid_r[...], 0.0)), split(mid_f[...]), first)
        high_w = dot3(split(jnp.where(rows < count_ref[0], high_r[...], 0.0)), split(high_f[...]), first)
        wm_top[...], wm_rest[...] = split(mid_w)
        w_top[...], w_rest[...] = split(high_w)
        low_w = split(low_w)
        parts = []
        for c in range(low_chunks):
            at = (low_chunks - 1 - c) * LANES
            frames = (fl_top[at : at + LANES, :LANES], fl_rest[at : at + LANES, :LANES])
            parts.append(dot3(low_w, frames))
        low = jnp.concatenate(parts, axis=1)
        time = y * low_here - (HALF_TAPS + 1) + lax.broadcasted_iota(jnp.int32, low.shape, 1)
        low = split(jnp.where((time >= 0) & (time < low_total), low, 0.0))
        cols = p_top.shape[1]
        for start in range(0, cols, WIDE):
            size = min(WIDE, cols - start)
            at = (mid_chunks - taps_mid // LANES - start // LANES) * LANES
            frames = (fm_top[at : at + taps_mid, :size], fm_rest[at : at + taps_mid, :size])
            value = dot3((wm_top[...], wm_rest[...]), frames)
            base, lead = start // g_ref.shape[1] * LANES, start % g_ref.shape[1]
            pieces = tuple(v[:, base : base + WIDE] for v in low)
            value += dot3(pieces, (g_top[:, lead : lead + size], g_rest[:, lead : lead + size]))
            time = y * mid_here - HALF_TAPS + start + lax.broadcasted_iota(jnp.int32, value.shape, 1)
            top, rest = split(jnp.where((time >= 0) & (time < mid_total), value, 0.0))
            p_top[:, start : start + size] = top
            p_rest[:, start : start + size] = rest

    base = pl.multiple_of(step * (width // RATIO), LANES)
    pieces = (p_top[:, pl.ds(base, WIDE)], p_rest[:, pl.ds(base, WIDE)])
    for start in range(0, width, WIDE):
        at = (high_chunks - taps // LANES - start // LANES - step * (width // LANES)) * LANES
        rows = pl.ds(pl.multiple_of(at, LANES), taps)
        value = dot3((w_top[...], w_rest[...]), (fh_top[rows, :], fh_rest[rows, :]))
        tile = slice(start, start + WIDE)
        out_ref[0, :, tile] = value + dot3(pieces, (g_top[:, tile], g_rest[:, tile]))


def compute(dims, count, filters, recons, strains):
    low_here, mid_here, low_total, mid_total = dims
    basis, _, tmpl = recons[0].shape
    taps_low, taps_mid, taps = (f.shape[1] for f in filters)
    samples = strains[3].shape[0] * LANES
    width = RATIO * LANES
    cols = mid_here + LANES
    g = jnp.asarray(upsample_matrix(WIDE, width))
    half = jnp.bfloat16

    def frames(rows):
        return [pltpu.VMEM((rows, WIDE), half)] * 2

    return pl.pallas_call(
        functools.partial(compute_kernel, dims),
        grid=(samples // width,),
        out_shape=jax.ShapeDtypeStruct((1, tmpl, samples), jnp.float32),
        in_specs=[pl.BlockSpec(memory_space=pltpu.SMEM)]
        + [pl.BlockSpec(memory_space=pltpu.VMEM)] * 8
        + [pl.BlockSpec(memory_space=pl.ANY)] * 3,
        out_specs=pl.BlockSpec((1, tmpl, width), lambda i: (0, 0, i)),
        scratch_shapes=[pltpu.VMEM((basis, tmpl), jnp.float32)] * 3
        + [pltpu.SemaphoreType.DMA((3,)), pltpu.VMEM(((samples + taps) // LANES, LANES), jnp.float32)]
        + frames(low_here + 2 * LANES + taps_low) + frames(cols + taps_mid) + frames(samples + taps)
        + [pltpu.VMEM((tmpl, taps), half)] * 2
        + [pltpu.VMEM((tmpl, taps_mid), half)] * 2
        + [pltpu.VMEM((tmpl, cols), half)] * 2
        + [pltpu.VMEM((WIDE, width), half)] * 2,
        compiler_params=pltpu.CompilerParams(vmem_limit_bytes=60 * 1024 * 1024),
        name="filter_templates",
    )(count, *filters, *strains, g, *recons)


def local(
    sizes, strain_high, strain_mid, strain_low, filters_high, filters_mid, filters_low,
    recon_high, recon_mid, recon_low, basis_count,
):
    slices = sizes[2]
    n_mid, n_low = strain_mid.shape[0], strain_low.shape[0]
    s_low, s_mid, s_high = (s.reshape(-1, LANES) for s in (strain_low, strain_mid, strain_high))
    low, mid, high, x_low, x_mid, x_prev = gather(
        sizes, filters_low, filters_mid, filters_high, s_low, s_mid, s_high
    )

    def flat(f):
        return f.reshape(-1, f.shape[2])

    return compute(
        (n_low, n_mid, n_low * slices, n_mid * slices), basis_count,
        (flat(low), flat(mid), flat(high)),
        (recon_low, recon_mid, recon_high),
        (x_low, flat(x_mid), x_prev, s_high),
    )


def solution(mesh):
    sizes = tuple(mesh.shape[name] for name in ("band", "tmpl", "tm"))
    in_specs = (
        P("tm"), P("tm"), P("tm"),
        P("tmpl", None), P("tmpl", None), P("tmpl", None),
        P(None, None, "tmpl"), P(None, None, "tmpl"), P(None, None, "tmpl"),
        P(),
    )
    return jax.shard_map(
        functools.partial(local, sizes), mesh=mesh, in_specs=in_specs,
        out_specs=P("band", "tmpl", "tm"), check_vma=False,
    )
```

```python
import functools
import math

import jax
import jax.numpy as jnp
import numpy as np
from jax import lax
from jax.experimental import pallas as pl
from jax.experimental.pallas import tpu as pltpu
from jax.sharding import PartitionSpec as P

RATIO = 8
HALF_TAPS = 8
LANES = 128
WIDE = 256
MESH = pl.DeviceIdType.MESH


def upsample_matrix(rows, cols):
    u = np.arange(rows)[:, None]
    v = np.arange(cols)[None, :]
    lag = u - v // RATIO
    offset = (v % RATIO) / RATIO - (lag - HALF_TAPS)
    value = np.sinc(offset) * (0.5 + 0.5 * np.cos(np.pi * offset / (HALF_TAPS + 1)))
    return np.where((lag >= 0) & (lag < 2 * HALF_TAPS), value, 0.0).astype(np.float32)


def gather_kernel(
    sizes, count_ref, low_ref, mid_ref, high_ref, sl_ref, sm_ref, sh_ref, g_top, g_rest,
    recon_low, recon_mid, recon_high,
    w_top, w_rest, p_top, p_rest, frames_top, frames_rest,
    low_all, mid_all, high_all, sl_all, sm_all, sh_prev,
    low_r, mid_r, high_r, recon_sem, frame_sem, x_full,
    fl_top, fl_rest, fm_top, fm_rest, fh_top, fh_rest,
    strain_send, strain_recv, lz_send, lz_recv, lx_send, lx_recv,
    z_send, z_recv, x_send, x_recv, y_send, y_recv, d_send, d_recv, c_send, c_recv,
):
    bands, peers, slices, lines, parts = sizes
    rings = peers // lines
    b, p, y = lax.axis_index("band"), lax.axis_index("tmpl"), lax.axis_index("tm")
    z, x = p // lines, p % lines
    part = y % parts

    def along_z(k):
        return (b, ((z + k) % rings) * lines + x, y)

    def along_y(m):
        return (b, p, y - part + (part + m) % parts)

    across = (b, z * lines + (x + 1) % lines, y)
    sibling = (1 - b, p, y)
    barrier = pltpu.get_barrier_semaphore()
    others = [along_z(k) for k in range(1, rings)] + [sibling]
    others += [(b, p, (y + k) % slices) for k in range(1, slices)]
    if lines > 1:
        others += [across]
    for device in others:
        pl.semaphore_signal(barrier, inc=1, device_id=device, device_id_type=MESH)
    pl.semaphore_wait(barrier, len(others))

    sent, strains, landed = [], [], ([], [])

    def send(src, dst, sems, at, device):
        copy = pltpu.make_async_remote_copy(
            src_ref=src, dst_ref=dst, send_sem=sems[0].at[at], recv_sem=sems[1].at[at],
            device_id=device, device_id_type=MESH,
        )
        copy.start()
        sent.append(copy)
        return copy

    strain = (strain_send, strain_recv)
    for k in range(1, slices):
        device = (b, p, (y + k) % slices)
        strains.append(send(sl_ref, sl_all.at[2 + y], strain, (0, k), device))
        strains.append(send(sm_ref, sm_all.at[2 + y], strain, (1, k), device))
    if slices > 1:
        tail = sh_prev.shape[0]
        last = sh_ref.at[pl.ds(sh_ref.shape[0] - tail, tail)]
        strains.append(send(last, sh_prev, strain, (2, 1), (b, p, (y + 1) % slices)))

    arrays = ((mid_ref, mid_all), (high_ref, high_all))
    size = [ref.shape[1] // (bands * parts) for ref, _ in arrays]

    def cols(a, m=0):
        start = (b * parts + (part + m) % parts) * size[a]
        return pl.ds(pl.multiple_of(start, LANES), size[a])

    def shard(k, other=0):
        return ((z + rings - k) % rings) * lines + (x + other) % lines

    low_z = {k: send(low_ref, low_all.at[p], (lz_send, lz_recv), k, along_z(k)) for k in range(1, rings)}
    from_z, from_x, from_y, from_d = {}, {}, {}, {}
    low_x = {}
    if lines > 1:
        low_x[0] = send(low_ref, low_all.at[p], (lx_send, lx_recv), 0, across)
    for a, (ref, full) in enumerate(arrays):
        for k in range(1, rings):
            from_z[a, k] = send(
                ref.at[:, cols(a)], full.at[p, :, cols(a)], (z_send, z_recv), (a, k), along_z(k)
            )
        if lines > 1:
            for m in range(parts):
                piece = send(
                    ref.at[:, cols(a, m)], full.at[p, :, cols(a, m)],
                    (x_send, x_recv) if m == 0 else (d_send, d_recv), (a, m, 0), across,
                )
                (from_x if m == 0 else from_d)[a, m, 0] = piece
    low_all[p] = low_ref[...]
    mid_all[p] = mid_ref[...]
    high_all[p] = high_ref[...]
    for ref, value in ((sl_all, sl_ref), (sm_all, sm_ref)):
        zero = jnp.zeros(value.shape, jnp.float32)
        ref[0] = zero
        ref[1] = zero
        ref[slices + 2] = zero
        ref[slices + 3] = zero
        ref[2 + y] = value[...]
    if slices == 1:
        sh_prev[...] = jnp.zeros(sh_prev.shape, jnp.float32)

    count = [0]

    def pass_on(a, view):
        at = (a, count[0])
        count[0] += 1
        landed[a].append(send(view, view, (c_send, c_recv), at, sibling))

    recons = []
    for i, (src, dst) in enumerate(((recon_low, low_r), (recon_mid, mid_r), (recon_high, high_r))):
        copy = pltpu.make_async_copy(src.at[:, b, :], dst, recon_sem.at[i])
        copy.start()
        recons.append(copy)
    for copy in strains:
        copy.wait_recv()
    before = sh_prev.shape[0]
    x_full[:before] = jnp.where(y > 0, sh_prev[...], 0.0)
    x_full[before:] = sh_ref[...]
    chunks = fh_top.shape[0] // LANES - 1
    stride = -(-chunks // 3)
    stores = []

    def frames_part(i):
        first, last = i * stride, min(chunks, (i + 1) * stride)
        fill_frames(lambda r: x_full[pl.ds(r, 1), :], fh_top, fh_rest, chunks, first, last)
        low, high = (chunks + 1 - last) * LANES if last < chunks else 0, (chunks + 1 - first) * LANES
        for j, (src, dst) in enumerate(((fh_top, frames_top), (fh_rest, frames_rest))):
            rows = pl.ds(low, high - low)
            copy = pltpu.make_async_copy(src.at[rows], dst.at[rows], frame_sem.at[i, j])
            copy.start()
            stores.append(copy)

    frames_part(0)
    for k in range(1, rings):
        low_z[k].wait_recv()
        if lines > 1:
            view = low_all.at[shard(k)]
            low_x[k] = send(view, view, (lx_send, lx_recv), k, across)
    for a, (_, full) in enumerate(arrays):
        count[0] = 0
        for k in range(1, rings):
            from_z[a, k].wait_recv()
            view = full.at[shard(k), :, cols(a)]
            if lines > 1:
                from_x[a, 0, k] = send(view, view, (x_send, x_recv), (a, 0, k), across)
            for m in range(1, parts):
                from_y[a, m, k] = send(view, view, (y_send, y_recv), (a, m, k), along_y(m))
            pass_on(a, view)
    base = count[0]
    frames_part(1)
    for a, (_, full) in enumerate(arrays):
        count[0] = base
        for k in range(rings):
            if lines > 1:
                from_x[a, 0, k].wait_recv()
                view = full.at[shard(k, 1), :, cols(a)]
                if k > 0:
                    for m in range(1, parts):
                        from_d[a, m, k] = send(view, view, (d_send, d_recv), (a, m, k), along_y(m))
                pass_on(a, view)
            for m in range(1, parts):
                if k == 0:
                    continue
                from_y[a, m, k].wait_recv()
                view = full.at[shard(k), :, cols(a, parts - m)]
                pass_on(a, view)
    base = count[0]
    frames_part(2)

    def last_pieces(a, full):
        count[0] = base
        for k in range(rings):
            for m in range(1, parts):
                if lines > 1:
                    from_d[a, m, k].wait_recv()
                    shift = m if k == 0 else parts - m
                    pass_on(a, full.at[shard(k, 1), :, cols(a, shift)])

    low_here, mid_here, low_total, mid_total = bounds(sl_ref, sm_ref, slices)
    taps_low, taps_mid = low_ref.shape[1], mid_ref.shape[1]
    low_chunks, mid_chunks = (r.shape[0] // LANES - 1 for r in (fl_top, fm_top))
    rows_mid = mid_here // LANES

    def low_row(r):
        return sl_all[y + 1 - taps_low // LANES + r]

    def mid_row(r):
        at = r + (y + 2) * rows_mid - taps_mid // LANES - 1
        return sm_all[at // rows_mid, pl.ds(at % rows_mid, 1), :]

    fill_frames(shifted(low_row, HALF_TAPS + 1), fl_top, fl_rest, low_chunks)
    fill_frames(shifted(mid_row, HALF_TAPS), fm_top, fm_rest, mid_chunks)
    for copy in recons:
        copy.wait()
    last_pieces(*(0, mid_all))
    for copy in low_x.values():
        copy.wait_recv()
    low_w = split(template_filters(low_r, low_all, count_ref[2]))
    parts_low = []
    for c in range(low_chunks):
        at = (low_chunks - 1 - c) * LANES
        parts_low.append(dot3(low_w, (fl_top[at : at + LANES, :LANES], fl_rest[at : at + LANES, :LANES])))
    low = jnp.concatenate(parts_low, axis=1)
    time = y * low_here - (HALF_TAPS + 1) + lax.broadcasted_iota(jnp.int32, low.shape, 1)
    low = split(jnp.where((time >= 0) & (time < low_total), low, 0.0))
    for copy in landed[0]:
        copy.wait_recv()
    mid_w = split(template_filters(mid_r, mid_all, count_ref[1]))
    last_pieces(*(1, high_all))
    width, columns = g_top.shape[1], p_top.shape[1]
    for start in range(0, columns, WIDE):
        size_here = min(WIDE, columns - start)
        at = (mid_chunks - taps_mid // LANES - start // LANES) * LANES
        frames = (fm_top[at : at + taps_mid, :size_here], fm_rest[at : at + taps_mid, :size_here])
        value = dot3(mid_w, frames)
        base_col, lead = start // width * LANES, start % width
        tile = slice(lead, lead + size_here)
        pieces = tuple(v[:, base_col : base_col + WIDE] for v in low)
        value += dot3(pieces, (g_top[:, tile], g_rest[:, tile]))
        time = y * mid_here - HALF_TAPS + start + lax.broadcasted_iota(jnp.int32, value.shape, 1)
        top, rest = split(jnp.where((time >= 0) & (time < mid_total), value, 0.0))
        p_top[:, start : start + size_here] = top
        p_rest[:, start : start + size_here] = rest
    for copy in landed[1]:
        copy.wait_recv()
    w_top[...], w_rest[...] = split(template_filters(high_r, high_all, count_ref[0]))
    for copy in sent:
        copy.wait_send()
    for copy in stores:
        copy.wait()


def bounds(s_low, s_mid, slices):
    low, mid = s_low.shape[0] * LANES, s_mid.shape[0] * LANES
    return low, mid, low * slices, mid * slices


def template_filters(recon_ref, full, count):
    peers, rows, taps = full.shape
    first = (((0,), (0,)), ((), ()))
    index = lax.broadcasted_iota(jnp.int32, recon_ref.shape, 0)
    recon = jnp.where(index < count, recon_ref[...], 0.0)
    if rows % 8 == 0:
        return dot3(split(recon), split(full[...].reshape(peers * rows, taps)), first)
    total = 0.0
    for p in range(peers):
        total += dot3(split(recon[p * rows : (p + 1) * rows]), split(full[p]), first)
    return total


def gather(sizes, count, filters, strains, g, recons):
    low, mid, high = filters
    s_low, s_mid, s_high = strains
    bands, peers, slices = sizes
    lines = 2 if peers % 2 == 0 else 1
    rings = peers // lines
    parts = math.gcd(slices, min(mid.shape[1], high.shape[1]) // (bands * LANES))
    f32, half = jnp.float32, jnp.bfloat16
    basis, _, tmpl = recons[0].shape
    taps_low, taps_mid, taps = (f.shape[1] for f in filters)
    low_here, mid_here, _, _ = bounds(s_low, s_mid, slices)
    samples = s_high.shape[0] * LANES
    columns = mid_here + LANES
    vmem = pl.BlockSpec(memory_space=pltpu.VMEM)
    anywhere = pl.BlockSpec(memory_space=pl.ANY)
    dma = pltpu.SemaphoreType.DMA

    def two(*dims):
        return [dma(dims)] * 2

    def frames(rows):
        return [pltpu.VMEM((rows, WIDE), half)] * 2

    return pl.pallas_call(
        functools.partial(gather_kernel, (bands, peers, slices, lines, parts)),
        out_shape=[jax.ShapeDtypeStruct((tmpl, taps), half)] * 2
        + [jax.ShapeDtypeStruct((tmpl, columns), half)] * 2
        + [jax.ShapeDtypeStruct((samples + taps, WIDE), half)] * 2,
        in_specs=[pl.BlockSpec(memory_space=pltpu.SMEM)] + [vmem] * 8 + [anywhere] * 3,
        out_specs=[vmem] * 4 + [anywhere] * 2,
        scratch_shapes=[pltpu.VMEM((peers,) + a.shape, f32) for a in filters]
        + [pltpu.VMEM((slices + 4,) + a.shape, f32) for a in (s_low, s_mid)]
        + [pltpu.VMEM((taps // LANES, LANES), f32)]
        + [pltpu.VMEM((basis, tmpl), f32)] * 3
        + [dma((3,)), dma((3, 2)), pltpu.VMEM(((samples + taps) // LANES, LANES), f32)]
        + frames(low_here + 2 * LANES + taps_low) + frames(columns + taps_mid) + frames(samples + taps)
        + two(3, slices) + two(rings) + two(rings) + two(2, rings)
        + two(2, parts, rings) * 3 + two(2, peers * parts),
        compiler_params=pltpu.CompilerParams(
            collective_id=0, has_side_effects=True, vmem_limit_bytes=60 * 1024 * 1024
        ),
        name="gather_filters",
    )(count, *filters, *strains, *g, *recons)


def split(value):
    top = value.astype(jnp.bfloat16)
    return top, (value - top.astype(jnp.float32)).astype(jnp.bfloat16)


def dot3(a, b, dims=(((1,), (0,)), ((), ()))):
    def one(u, v):
        return lax.dot_general(u, v, dims, preferred_element_type=jnp.float32)

    return one(a[0], b[0]) + one(a[0], b[1]) + one(a[1], b[0])


def staggered(row):
    return pltpu.roll(jnp.broadcast_to(row, (LANES, LANES)), 0, 1, stride=1, stride_axis=0)


def shifted(read, by):
    lane = lax.broadcasted_iota(jnp.int32, (1, LANES), 1)

    def row(r):
        late = [pltpu.roll(read(r + i), by, 1) for i in range(2)]
        return jnp.where(lane >= by, late[1], late[0])

    return row


def fill_frames(row, top_ref, rest_ref, chunks, first=0, last=None):
    lane = lax.broadcasted_iota(jnp.int32, (LANES, LANES), 1)
    lag = lax.broadcasted_iota(jnp.int32, (LANES, LANES), 0)

    def step(c, before):
        now = staggered(row(c + 1))
        top, rest = split(jnp.where(lane >= lag, now, before))
        left = pl.multiple_of((chunks - 1 - c) * LANES, LANES)
        right = pl.multiple_of((chunks - c) * LANES, LANES)
        for ref, value in ((top_ref, top), (rest_ref, rest)):
            ref[pl.ds(left, LANES), :LANES] = value
            ref[pl.ds(right, LANES), LANES:] = value
        return now

    lax.fori_loop(first, chunks if last is None else last, step, staggered(row(first)))


def compute_kernel(
    w_top, w_rest, p_top, p_rest, g_top, g_rest, frames_top, frames_rest,
    out_ref, fh_top, fh_rest, frame_sem,
):
    step = pl.program_id(0)
    blocks = pl.num_programs(0)
    taps = w_top.shape[1]
    width = out_ref.shape[2]
    chunks = fh_top.shape[0] // LANES - 1

    def block(j):
        rows = pl.ds(pl.multiple_of(j * width, width), width)
        return [
            pltpu.make_async_copy(src.at[rows], dst.at[rows], frame_sem.at[j, i])
            for i, (src, dst) in enumerate(((frames_top, fh_top), (frames_rest, fh_rest)))
        ]

    total = fh_top.shape[0] // width
    ahead = taps // width

    @pl.when(step == 0)
    def _():
        for j in reversed(range(total)):
            for copy in block(j):
                copy.start()
        for j in range(total - ahead, total):
            for copy in block(j):
                copy.wait()

    for copy in block(blocks - 1 - step):
        copy.wait()
    base = pl.multiple_of(step * (width // RATIO), LANES)
    pieces = (p_top[:, pl.ds(base, WIDE)], p_rest[:, pl.ds(base, WIDE)])
    for start in range(0, width, WIDE):
        at = (chunks - taps // LANES - start // LANES - step * (width // LANES)) * LANES
        rows = pl.ds(pl.multiple_of(at, LANES), taps)
        value = dot3((w_top[...], w_rest[...]), (fh_top[rows, :], fh_rest[rows, :]))
        tile = slice(start, start + WIDE)
        out_ref[0, :, tile] = value + dot3(pieces, (g_top[:, tile], g_rest[:, tile]))


def compute(w, p, g, frames):
    tmpl, taps = w[0].shape
    rows = frames[0].shape[0]
    samples = rows - taps
    width = g[0].shape[1]
    vmem = pl.BlockSpec(memory_space=pltpu.VMEM)
    return pl.pallas_call(
        compute_kernel,
        grid=(samples // width,),
        out_shape=jax.ShapeDtypeStruct((1, tmpl, samples), jnp.float32),
        in_specs=[vmem] * 6 + [pl.BlockSpec(memory_space=pl.ANY)] * 2,
        out_specs=pl.BlockSpec((1, tmpl, width), lambda i: (0, 0, i)),
        scratch_shapes=[pltpu.VMEM((rows, WIDE), jnp.bfloat16)] * 2
        + [pltpu.SemaphoreType.DMA((rows // width, 2))],
        compiler_params=pltpu.CompilerParams(vmem_limit_bytes=60 * 1024 * 1024),
        name="filter_templates",
    )(*w, *p, *g, *frames)


def local(
    sizes, strain_high, strain_mid, strain_low, filters_high, filters_mid, filters_low,
    recon_high, recon_mid, recon_low, basis_count,
):
    matrix = upsample_matrix(WIDE, RATIO * LANES)
    top = matrix.astype(jnp.bfloat16)
    rest = (matrix - top.astype(np.float32)).astype(jnp.bfloat16)
    g = (jnp.asarray(top), jnp.asarray(rest))
    strains = [s.reshape(-1, LANES) for s in (strain_low, strain_mid, strain_high)]
    out = gather(
        sizes, basis_count, (filters_low, filters_mid, filters_high), strains, g,
        (recon_low, recon_mid, recon_high),
    )
    return compute(out[:2], out[2:4], g, out[4:])


def solution(mesh):
    sizes = tuple(mesh.shape[name] for name in ("band", "tmpl", "tm"))
    in_specs = (
        P("tm"), P("tm"), P("tm"),
        P("tmpl", None), P("tmpl", None), P("tmpl", None),
        P(None, None, "tmpl"), P(None, None, "tmpl"), P(None, None, "tmpl"),
        P(),
    )
    return jax.shard_map(
        functools.partial(local, sizes), mesh=mesh, in_specs=in_specs,
        out_specs=P("band", "tmpl", "tm"), check_vma=False,
    )
```

```python
import functools
import math

import jax
import jax.numpy as jnp
import numpy as np
from jax import lax
from jax.experimental import pallas as pl
from jax.experimental.pallas import tpu as pltpu
from jax.sharding import PartitionSpec as P

RATIO = 8
HALF_TAPS = 8
LANES = 128
WIDE = 256
MESH = pl.DeviceIdType.MESH


def upsample_matrix(rows, cols):
    u = np.arange(rows)[:, None]
    v = np.arange(cols)[None, :]
    lag = u - v // RATIO
    offset = (v % RATIO) / RATIO - (lag - HALF_TAPS)
    value = np.sinc(offset) * (0.5 + 0.5 * np.cos(np.pi * offset / (HALF_TAPS + 1)))
    return np.where((lag >= 0) & (lag < 2 * HALF_TAPS), value, 0.0).astype(np.float32)


def gather_kernel(
    sizes, count_ref, low_ref, mid_ref, high_ref, sl_ref, sm_ref, sh_ref, g_top, g_rest,
    recon_low, recon_mid, recon_high,
    w_top, w_rest, p_top, p_rest, frames_top, frames_rest,
    low_all, mid_all, high_all, sl_all, sm_all, sh_prev,
    low_r, mid_r, high_r, recon_sem, frame_sem, x_full,
    fl_top, fl_rest, fm_top, fm_rest, fh_top, fh_rest,
    strain_send, strain_recv, lz_send, lz_recv, lx_send, lx_recv,
    z_send, z_recv, x_send, x_recv, y_send, y_recv, d_send, d_recv, c_send, c_recv,
):
    bands, peers, slices, lines, parts = sizes
    rings = peers // lines
    b, p, y = lax.axis_index("band"), lax.axis_index("tmpl"), lax.axis_index("tm")
    z, x = p // lines, p % lines
    part = y % parts

    def along_z(k):
        return (b, ((z + k) % rings) * lines + x, y)

    def along_y(m):
        return (b, p, y - part + (part + m) % parts)

    across = (b, z * lines + (x + 1) % lines, y)
    sibling = (1 - b, p, y)
    barrier = pltpu.get_barrier_semaphore()
    others = [along_z(k) for k in range(1, rings)] + [sibling]
    others += [(b, p, (y + k) % slices) for k in range(1, slices)]
    if lines > 1:
        others += [across]
    for device in others:
        pl.semaphore_signal(barrier, inc=1, device_id=device, device_id_type=MESH)
    pl.semaphore_wait(barrier, len(others))

    sent, strains, landed = [], [], ([], [])

    def send(src, dst, sems, at, device):
        copy = pltpu.make_async_remote_copy(
            src_ref=src, dst_ref=dst, send_sem=sems[0].at[at], recv_sem=sems[1].at[at],
            device_id=device, device_id_type=MESH,
        )
        copy.start()
        sent.append(copy)
        return copy

    strain = (strain_send, strain_recv)
    for k in range(1, slices):
        device = (b, p, (y + k) % slices)
        strains.append(send(sl_ref, sl_all.at[2 + y], strain, (0, k), device))
        strains.append(send(sm_ref, sm_all.at[2 + y], strain, (1, k), device))
    if slices > 1:
        tail = sh_prev.shape[0]
        last = sh_ref.at[pl.ds(sh_ref.shape[0] - tail, tail)]
        strains.append(send(last, sh_prev, strain, (2, 1), (b, p, (y + 1) % slices)))

    arrays = ((mid_ref, mid_all), (high_ref, high_all))
    size = [ref.shape[1] // (bands * parts) for ref, _ in arrays]

    def cols(a, m=0):
        start = (b * parts + (part + m) % parts) * size[a]
        return pl.ds(pl.multiple_of(start, LANES), size[a])

    def shard(k, other=0):
        return ((z + rings - k) % rings) * lines + (x + other) % lines

    low_z = {k: send(low_ref, low_all.at[p], (lz_send, lz_recv), k, along_z(k)) for k in range(1, rings)}
    from_z, from_x, from_y, from_d = {}, {}, {}, {}
    low_x = {}
    if lines > 1:
        low_x[0] = send(low_ref, low_all.at[p], (lx_send, lx_recv), 0, across)
    for a, (ref, full) in enumerate(arrays):
        for k in range(1, rings):
            from_z[a, k] = send(
                ref.at[:, cols(a)], full.at[p, :, cols(a)], (z_send, z_recv), (a, k), along_z(k)
            )
        if lines > 1:
            for m in range(parts):
                piece = send(
                    ref.at[:, cols(a, m)], full.at[p, :, cols(a, m)],
                    (x_send, x_recv) if m == 0 else (d_send, d_recv), (a, m, 0), across,
                )
                (from_x if m == 0 else from_d)[a, m, 0] = piece
    low_all[p] = low_ref[...]
    mid_all[p] = mid_ref[...]
    high_all[p] = high_ref[...]
    for ref, value in ((sl_all, sl_ref), (sm_all, sm_ref)):
        zero = jnp.zeros(value.shape, jnp.float32)
        ref[0] = zero
        ref[1] = zero
        ref[slices + 2] = zero
        ref[slices + 3] = zero
        ref[2 + y] = value[...]
    if slices == 1:
        sh_prev[...] = jnp.zeros(sh_prev.shape, jnp.float32)

    count = [0]

    def pass_on(a, view):
        at = (a, count[0])
        count[0] += 1
        landed[a].append(send(view, view, (c_send, c_recv), at, sibling))

    recons = []
    for i, (src, dst) in enumerate(((recon_low, low_r), (recon_mid, mid_r), (recon_high, high_r))):
        copy = pltpu.make_async_copy(src.at[:, b, :], dst, recon_sem.at[i])
        copy.start()
        recons.append(copy)
    for copy in strains:
        copy.wait_recv()
    before = sh_prev.shape[0]
    x_full[:before] = jnp.where(y > 0, sh_prev[...], 0.0)
    x_full[before:] = sh_ref[...]
    chunks = fh_top.shape[0] // LANES - 1
    stride = -(-chunks // 6)
    stores = []

    def frames_part(i):
        first, last = i * stride, min(chunks, (i + 1) * stride)
        fill_frames(lambda r: x_full[pl.ds(r, 1), :], fh_top, fh_rest, chunks, first, last)
        low, high = (chunks + 1 - last) * LANES if last < chunks else 0, (chunks + 1 - first) * LANES
        for j, (src, dst) in enumerate(((fh_top, frames_top), (fh_rest, frames_rest))):
            rows = pl.ds(low, high - low)
            copy = pltpu.make_async_copy(src.at[rows], dst.at[rows], frame_sem.at[i, j])
            copy.start()
            stores.append(copy)

    frames_part(0)
    for k in range(1, rings):
        low_z[k].wait_recv()
        if lines > 1:
            view = low_all.at[shard(k)]
            low_x[k] = send(view, view, (lx_send, lx_recv), k, across)
    for a, (_, full) in enumerate(arrays):
        count[0] = 0
        for k in range(1, rings):
            from_z[a, k].wait_recv()
            view = full.at[shard(k), :, cols(a)]
            if lines > 1:
                from_x[a, 0, k] = send(view, view, (x_send, x_recv), (a, 0, k), across)
            for m in range(1, parts):
                from_y[a, m, k] = send(view, view, (y_send, y_recv), (a, m, k), along_y(m))
            pass_on(a, view)
        frames_part(1 + a)
    base = count[0]
    for a, (_, full) in enumerate(arrays):
        count[0] = base
        for k in range(rings):
            if lines > 1:
                from_x[a, 0, k].wait_recv()
                view = full.at[shard(k, 1), :, cols(a)]
                if k > 0:
                    for m in range(1, parts):
                        from_d[a, m, k] = send(view, view, (d_send, d_recv), (a, m, k), along_y(m))
                pass_on(a, view)
            for m in range(1, parts):
                if k == 0:
                    continue
                from_y[a, m, k].wait_recv()
                view = full.at[shard(k), :, cols(a, parts - m)]
                pass_on(a, view)
        frames_part(3 + a)
    base = count[0]
    frames_part(5)

    def last_pieces(a, full):
        count[0] = base
        for k in range(rings):
            for m in range(1, parts):
                if lines > 1:
                    from_d[a, m, k].wait_recv()
                    shift = m if k == 0 else parts - m
                    pass_on(a, full.at[shard(k, 1), :, cols(a, shift)])

    low_here, mid_here, low_total, mid_total = bounds(sl_ref, sm_ref, slices)
    taps_low, taps_mid = low_ref.shape[1], mid_ref.shape[1]
    low_chunks, mid_chunks = (r.shape[0] // LANES - 1 for r in (fl_top, fm_top))
    rows_mid = mid_here // LANES

    def low_row(r):
        return sl_all[y + 1 - taps_low // LANES + r]

    def mid_row(r):
        at = r + (y + 2) * rows_mid - taps_mid // LANES - 1
        return sm_all[at // rows_mid, pl.ds(at % rows_mid, 1), :]

    fill_frames(shifted(low_row, HALF_TAPS + 1), fl_top, fl_rest, low_chunks)
    fill_frames(shifted(mid_row, HALF_TAPS), fm_top, fm_rest, mid_chunks)
    for copy in recons:
        copy.wait()
    last_pieces(*(0, mid_all))
    for copy in low_x.values():
        copy.wait_recv()
    low_w = split(template_filters(low_r, low_all, count_ref[2]))
    parts_low = []
    for c in range(low_chunks):
        at = (low_chunks - 1 - c) * LANES
        parts_low.append(dot3(low_w, (fl_top[at : at + LANES, :LANES], fl_rest[at : at + LANES, :LANES])))
    low = jnp.concatenate(parts_low, axis=1)
    time = y * low_here - (HALF_TAPS + 1) + lax.broadcasted_iota(jnp.int32, low.shape, 1)
    low = split(jnp.where((time >= 0) & (time < low_total), low, 0.0))
    for copy in landed[0]:
        copy.wait_recv()
    mid_w = split(template_filters(mid_r, mid_all, count_ref[1]))
    last_pieces(*(1, high_all))
    width, columns = g_top.shape[1], p_top.shape[1]
    for start in range(0, columns, WIDE):
        size_here = min(WIDE, columns - start)
        at = (mid_chunks - taps_mid // LANES - start // LANES) * LANES
        frames = (fm_top[at : at + taps_mid, :size_here], fm_rest[at : at + taps_mid, :size_here])
        value = dot3(mid_w, frames)
        base_col, lead = start // width * LANES, start % width
        tile = slice(lead, lead + size_here)
        pieces = tuple(v[:, base_col : base_col + WIDE] for v in low)
        value += dot3(pieces, (g_top[:, tile], g_rest[:, tile]))
        time = y * mid_here - HALF_TAPS + start + lax.broadcasted_iota(jnp.int32, value.shape, 1)
        top, rest = split(jnp.where((time >= 0) & (time < mid_total), value, 0.0))
        p_top[:, start : start + size_here] = top
        p_rest[:, start : start + size_here] = rest
    for copy in landed[1]:
        copy.wait_recv()
    w_top[...], w_rest[...] = split(template_filters(high_r, high_all, count_ref[0]))
    for copy in sent:
        copy.wait_send()
    for copy in stores:
        copy.wait()


def bounds(s_low, s_mid, slices):
    low, mid = s_low.shape[0] * LANES, s_mid.shape[0] * LANES
    return low, mid, low * slices, mid * slices


def template_filters(recon_ref, full, count):
    peers, rows, taps = full.shape
    first = (((0,), (0,)), ((), ()))
    index = lax.broadcasted_iota(jnp.int32, recon_ref.shape, 0)
    recon = jnp.where(index < count, recon_ref[...], 0.0)
    if rows % 8 == 0:
        return dot3(split(recon), split(full[...].reshape(peers * rows, taps)), first)
    total = 0.0
    for p in range(peers):
        total += dot3(split(recon[p * rows : (p + 1) * rows]), split(full[p]), first)
    return total


def gather(sizes, count, filters, strains, g, recons):
    low, mid, high = filters
    s_low, s_mid, s_high = strains
    bands, peers, slices = sizes
    lines = 2 if peers % 2 == 0 else 1
    rings = peers // lines
    parts = math.gcd(slices, min(mid.shape[1], high.shape[1]) // (bands * LANES))
    f32, half = jnp.float32, jnp.bfloat16
    basis, _, tmpl = recons[0].shape
    taps_low, taps_mid, taps = (f.shape[1] for f in filters)
    low_here, mid_here, _, _ = bounds(s_low, s_mid, slices)
    samples = s_high.shape[0] * LANES
    columns = mid_here + LANES
    vmem = pl.BlockSpec(memory_space=pltpu.VMEM)
    anywhere = pl.BlockSpec(memory_space=pl.ANY)
    dma = pltpu.SemaphoreType.DMA

    def two(*dims):
        return [dma(dims)] * 2

    def frames(rows):
        return [pltpu.VMEM((rows, WIDE), half)] * 2

    return pl.pallas_call(
        functools.partial(gather_kernel, (bands, peers, slices, lines, parts)),
        out_shape=[jax.ShapeDtypeStruct((tmpl, taps), half)] * 2
        + [jax.ShapeDtypeStruct((tmpl, columns), half)] * 2
        + [jax.ShapeDtypeStruct((samples + taps, WIDE), half)] * 2,
        in_specs=[pl.BlockSpec(memory_space=pltpu.SMEM)] + [vmem] * 8 + [anywhere] * 3,
        out_specs=[vmem] * 4 + [anywhere] * 2,
        scratch_shapes=[pltpu.VMEM((peers,) + a.shape, f32) for a in filters]
        + [pltpu.VMEM((slices + 4,) + a.shape, f32) for a in (s_low, s_mid)]
        + [pltpu.VMEM((taps // LANES, LANES), f32)]
        + [pltpu.VMEM((basis, tmpl), f32)] * 3
        + [dma((3,)), dma((6, 2)), pltpu.VMEM(((samples + taps) // LANES, LANES), f32)]
        + frames(low_here + 2 * LANES + taps_low) + frames(columns + taps_mid) + frames(samples + taps)
        + two(3, slices) + two(rings) + two(rings) + two(2, rings)
        + two(2, parts, rings) * 3 + two(2, peers * parts),
        compiler_params=pltpu.CompilerParams(
            collective_id=0, has_side_effects=True, vmem_limit_bytes=60 * 1024 * 1024
        ),
        name="gather_filters",
    )(count, *filters, *strains, *g, *recons)


def split(value):
    top = value.astype(jnp.bfloat16)
    return top, (value - top.astype(jnp.float32)).astype(jnp.bfloat16)


def dot3(a, b, dims=(((1,), (0,)), ((), ()))):
    def one(u, v):
        return lax.dot_general(u, v, dims, preferred_element_type=jnp.float32)

    return one(a[0], b[0]) + one(a[0], b[1]) + one(a[1], b[0])


def staggered(row):
    return pltpu.roll(jnp.broadcast_to(row, (LANES, LANES)), 0, 1, stride=1, stride_axis=0)


def shifted(read, by):
    lane = lax.broadcasted_iota(jnp.int32, (1, LANES), 1)

    def row(r):
        late = [pltpu.roll(read(r + i), by, 1) for i in range(2)]
        return jnp.where(lane >= by, late[1], late[0])

    return row


def fill_frames(row, top_ref, rest_ref, chunks, first=0, last=None):
    lane = lax.broadcasted_iota(jnp.int32, (LANES, LANES), 1)
    lag = lax.broadcasted_iota(jnp.int32, (LANES, LANES), 0)

    def step(c, before):
        now = staggered(row(c + 1))
        top, rest = split(jnp.where(lane >= lag, now, before))
        left = pl.multiple_of((chunks - 1 - c) * LANES, LANES)
        right = pl.multiple_of((chunks - c) * LANES, LANES)
        for ref, value in ((top_ref, top), (rest_ref, rest)):
            ref[pl.ds(left, LANES), :LANES] = value
            ref[pl.ds(right, LANES), LANES:] = value
        return now

    lax.fori_loop(first, chunks if last is None else last, step, staggered(row(first)))


def compute_kernel(
    w_top, w_rest, p_top, p_rest, g_top, g_rest, frames_top, frames_rest,
    out_ref, fh_top, fh_rest, frame_sem,
):
    step = pl.program_id(0)
    blocks = pl.num_programs(0)
    taps = w_top.shape[1]
    width = out_ref.shape[2]
    chunks = fh_top.shape[0] // LANES - 1

    def block(j):
        rows = pl.ds(pl.multiple_of(j * width, width), width)
        return [
            pltpu.make_async_copy(src.at[rows], dst.at[rows], frame_sem.at[j, i])
            for i, (src, dst) in enumerate(((frames_top, fh_top), (frames_rest, fh_rest)))
        ]

    total = fh_top.shape[0] // width
    ahead = taps // width

    @pl.when(step == 0)
    def _():
        for j in reversed(range(total)):
            for copy in block(j):
                copy.start()
        for j in range(total - ahead, total):
            for copy in block(j):
                copy.wait()

    for copy in block(blocks - 1 - step):
        copy.wait()
    base = pl.multiple_of(step * (width // RATIO), LANES)
    pieces = (p_top[:, pl.ds(base, WIDE)], p_rest[:, pl.ds(base, WIDE)])
    near = [piece[:, :LANES] for piece in pieces]
    stacked = jnp.concatenate(near, axis=1)
    for start in range(0, width, WIDE):
        at = (chunks - taps // LANES - start // LANES - step * (width // LANES)) * LANES
        rows = pl.ds(pl.multiple_of(at, LANES), taps)
        value = dot3((w_top[...], w_rest[...]), (fh_top[rows, :], fh_rest[rows, :]))
        tile = slice(start, start + WIDE)
        if (start + WIDE) // RATIO + 2 * HALF_TAPS <= LANES:
            top = g_top[:LANES, tile]
            value += jnp.dot(
                stacked, jnp.concatenate([top, top], axis=0), preferred_element_type=jnp.float32
            )
            value += jnp.dot(near[0], g_rest[:LANES, tile], preferred_element_type=jnp.float32)
        else:
            value += dot3(pieces, (g_top[:, tile], g_rest[:, tile]))
        out_ref[0, :, tile] = value


def compute(w, p, g, frames):
    tmpl, taps = w[0].shape
    rows = frames[0].shape[0]
    samples = rows - taps
    width = g[0].shape[1]
    vmem = pl.BlockSpec(memory_space=pltpu.VMEM)
    return pl.pallas_call(
        compute_kernel,
        grid=(samples // width,),
        out_shape=jax.ShapeDtypeStruct((1, tmpl, samples), jnp.float32),
        in_specs=[vmem] * 6 + [pl.BlockSpec(memory_space=pl.ANY)] * 2,
        out_specs=pl.BlockSpec((1, tmpl, width), lambda i: (0, 0, i)),
        scratch_shapes=[pltpu.VMEM((rows, WIDE), jnp.bfloat16)] * 2
        + [pltpu.SemaphoreType.DMA((rows // width, 2))],
        compiler_params=pltpu.CompilerParams(vmem_limit_bytes=60 * 1024 * 1024),
        name="filter_templates",
    )(*w, *p, *g, *frames)


def local(
    sizes, strain_high, strain_mid, strain_low, filters_high, filters_mid, filters_low,
    recon_high, recon_mid, recon_low, basis_count,
):
    matrix = upsample_matrix(WIDE, RATIO * LANES)
    top = matrix.astype(jnp.bfloat16)
    rest = (matrix - top.astype(np.float32)).astype(jnp.bfloat16)
    g = (jnp.asarray(top), jnp.asarray(rest))
    strains = [s.reshape(-1, LANES) for s in (strain_low, strain_mid, strain_high)]
    out = gather(
        sizes, basis_count, (filters_low, filters_mid, filters_high), strains, g,
        (recon_low, recon_mid, recon_high),
    )
    return compute(out[:2], out[2:4], g, out[4:])


def solution(mesh):
    sizes = tuple(mesh.shape[name] for name in ("band", "tmpl", "tm"))
    in_specs = (
        P("tm"), P("tm"), P("tm"),
        P("tmpl", None), P("tmpl", None), P("tmpl", None),
        P(None, None, "tmpl"), P(None, None, "tmpl"), P(None, None, "tmpl"),
        P(),
    )
    return jax.shard_map(
        functools.partial(local, sizes), mesh=mesh, in_specs=in_specs,
        out_specs=P("band", "tmpl", "tm"), check_vma=False,
    )
```

```python
import functools
import math

import jax
import jax.numpy as jnp
import numpy as np
from jax import lax
from jax.experimental import pallas as pl
from jax.experimental.pallas import tpu as pltpu
from jax.sharding import PartitionSpec as P

RATIO = 8
HALF_TAPS = 8
LANES = 128
WIDE = 256
MESH = pl.DeviceIdType.MESH


def upsample_matrix(rows, cols):
    u = np.arange(rows)[:, None]
    v = np.arange(cols)[None, :]
    lag = u - v // RATIO
    offset = (v % RATIO) / RATIO - (lag - HALF_TAPS)
    value = np.sinc(offset) * (0.5 + 0.5 * np.cos(np.pi * offset / (HALF_TAPS + 1)))
    return np.where((lag >= 0) & (lag < 2 * HALF_TAPS), value, 0.0).astype(np.float32)


def gather_kernel(
    sizes, count_ref, low_ref, mid_ref, high_ref, sl_ref, sm_ref, sh_ref, g_top, g_rest,
    recon_low, recon_mid, recon_high,
    w_top, w_rest, p_top, p_rest, frames_top, frames_rest,
    low_all, mid_all, high_all, sl_all, sm_all, sh_prev,
    low_r, mid_r, high_r, recon_sem, frame_sem, x_full,
    fl_top, fl_rest, fm_top, fm_rest, fh_top, fh_rest,
    strain_send, strain_recv, lz_send, lz_recv, lx_send, lx_recv,
    z_send, z_recv, x_send, x_recv, y_send, y_recv, d_send, d_recv, c_send, c_recv,
):
    bands, peers, slices, lines, parts = sizes
    rings = peers // lines
    b, p, y = lax.axis_index("band"), lax.axis_index("tmpl"), lax.axis_index("tm")
    z, x = p // lines, p % lines
    part = y % parts

    def along_z(k):
        return (b, ((z + k) % rings) * lines + x, y)

    def along_y(m):
        return (b, p, y - part + (part + m) % parts)

    across = (b, z * lines + (x + 1) % lines, y)
    sibling = (1 - b, p, y)
    barrier = pltpu.get_barrier_semaphore()
    others = [along_z(k) for k in range(1, rings)] + [sibling]
    others += [(b, p, (y + k) % slices) for k in range(1, slices)]
    if lines > 1:
        others += [across]
    for device in others:
        pl.semaphore_signal(barrier, inc=1, device_id=device, device_id_type=MESH)
    pl.semaphore_wait(barrier, len(others))

    sent, strains, landed = [], [], ([], [])

    def send(src, dst, sems, at, device):
        copy = pltpu.make_async_remote_copy(
            src_ref=src, dst_ref=dst, send_sem=sems[0].at[at], recv_sem=sems[1].at[at],
            device_id=device, device_id_type=MESH,
        )
        copy.start()
        sent.append(copy)
        return copy

    strain = (strain_send, strain_recv)
    for k in range(1, slices):
        device = (b, p, (y + k) % slices)
        strains.append(send(sl_ref, sl_all.at[2 + y], strain, (0, k), device))
        strains.append(send(sm_ref, sm_all.at[2 + y], strain, (1, k), device))
    if slices > 1:
        tail = sh_prev.shape[0]
        last = sh_ref.at[pl.ds(sh_ref.shape[0] - tail, tail)]
        strains.append(send(last, sh_prev, strain, (2, 1), (b, p, (y + 1) % slices)))

    arrays = ((mid_ref, mid_all), (high_ref, high_all))
    size = [ref.shape[1] // (bands * parts) for ref, _ in arrays]

    def cols(a, m=0):
        start = (b * parts + (part + m) % parts) * size[a]
        return pl.ds(pl.multiple_of(start, LANES), size[a])

    def shard(k, other=0):
        return ((z + rings - k) % rings) * lines + (x + other) % lines

    low_z = {k: send(low_ref, low_all.at[p], (lz_send, lz_recv), k, along_z(k)) for k in range(1, rings)}
    from_z, from_x, from_y, from_d = {}, {}, {}, {}
    low_x = {}
    if lines > 1:
        low_x[0] = send(low_ref, low_all.at[p], (lx_send, lx_recv), 0, across)
    for a, (ref, full) in enumerate(arrays):
        for k in range(1, rings):
            from_z[a, k] = send(
                ref.at[:, cols(a)], full.at[p, :, cols(a)], (z_send, z_recv), (a, k), along_z(k)
            )
        if lines > 1:
            for m in range(parts):
                piece = send(
                    ref.at[:, cols(a, m)], full.at[p, :, cols(a, m)],
                    (x_send, x_recv) if m == 0 else (d_send, d_recv), (a, m, 0), across,
                )
                (from_x if m == 0 else from_d)[a, m, 0] = piece
    low_all[p] = low_ref[...]
    mid_all[p] = mid_ref[...]
    high_all[p] = high_ref[...]
    for ref, value in ((sl_all, sl_ref), (sm_all, sm_ref)):
        zero = jnp.zeros(value.shape, jnp.float32)
        ref[0] = zero
        ref[1] = zero
        ref[slices + 2] = zero
        ref[slices + 3] = zero
        ref[2 + y] = value[...]
    if slices == 1:
        sh_prev[...] = jnp.zeros(sh_prev.shape, jnp.float32)

    count = [0]

    def pass_on(a, view):
        at = (a, count[0])
        count[0] += 1
        landed[a].append(send(view, view, (c_send, c_recv), at, sibling))

    recons = []
    for i, (src, dst) in enumerate(((recon_low, low_r), (recon_mid, mid_r), (recon_high, high_r))):
        copy = pltpu.make_async_copy(src.at[:, b, :], dst, recon_sem.at[i])
        copy.start()
        recons.append(copy)
    for copy in strains:
        copy.wait_recv()
    before = sh_prev.shape[0]
    x_full[:before] = jnp.where(y > 0, sh_prev[...], 0.0)
    x_full[before:] = sh_ref[...]
    chunks = fh_top.shape[0] // LANES - 1
    stride = -(-chunks // 3)
    stores = []

    def frames_part(i):
        first, last = i * stride, min(chunks, (i + 1) * stride)
        fill_frames(lambda r: x_full[pl.ds(r, 1), :], fh_top, fh_rest, chunks, first, last)
        low, high = (chunks + 1 - last) * LANES if last < chunks else 0, (chunks + 1 - first) * LANES
        for j, (src, dst) in enumerate(((fh_top, frames_top), (fh_rest, frames_rest))):
            rows = pl.ds(low, high - low)
            copy = pltpu.make_async_copy(src.at[rows], dst.at[rows], frame_sem.at[i, j])
            copy.start()
            stores.append(copy)

    frames_part(0)
    for k in range(1, rings):
        low_z[k].wait_recv()
        if lines > 1:
            view = low_all.at[shard(k)]
            low_x[k] = send(view, view, (lx_send, lx_recv), k, across)
    for a, (_, full) in enumerate(arrays):
        count[0] = 0
        for k in range(1, rings):
            from_z[a, k].wait_recv()
            view = full.at[shard(k), :, cols(a)]
            if lines > 1:
                from_x[a, 0, k] = send(view, view, (x_send, x_recv), (a, 0, k), across)
            for m in range(1, parts):
                from_y[a, m, k] = send(view, view, (y_send, y_recv), (a, m, k), along_y(m))
            pass_on(a, view)
    base = count[0]
    for a, (_, full) in enumerate(arrays):
        count[0] = base
        for k in range(rings):
            if lines > 1:
                from_x[a, 0, k].wait_recv()
                view = full.at[shard(k, 1), :, cols(a)]
                if k > 0:
                    for m in range(1, parts):
                        from_d[a, m, k] = send(view, view, (d_send, d_recv), (a, m, k), along_y(m))
                pass_on(a, view)
            for m in range(1, parts):
                if k == 0:
                    continue
                from_y[a, m, k].wait_recv()
                view = full.at[shard(k), :, cols(a, parts - m)]
                pass_on(a, view)
    base = count[0]
    frames_part(1)
    frames_part(2)

    def last_pieces(a, full):
        count[0] = base
        for k in range(rings):
            for m in range(1, parts):
                if lines > 1:
                    from_d[a, m, k].wait_recv()
                    shift = m if k == 0 else parts - m
                    pass_on(a, full.at[shard(k, 1), :, cols(a, shift)])

    low_here, mid_here, low_total, mid_total = bounds(sl_ref, sm_ref, slices)
    taps_low, taps_mid = low_ref.shape[1], mid_ref.shape[1]
    low_chunks, mid_chunks = (r.shape[0] // LANES - 1 for r in (fl_top, fm_top))
    rows_mid = mid_here // LANES

    def low_row(r):
        return sl_all[y + 1 - taps_low // LANES + r]

    def mid_row(r):
        at = r + (y + 2) * rows_mid - taps_mid // LANES - 1
        return sm_all[at // rows_mid, pl.ds(at % rows_mid, 1), :]

    fill_frames(shifted(low_row, HALF_TAPS + 1), fl_top, fl_rest, low_chunks)
    fill_frames(shifted(mid_row, HALF_TAPS), fm_top, fm_rest, mid_chunks)
    for copy in recons:
        copy.wait()
    last_pieces(*(0, mid_all))
    for copy in low_x.values():
        copy.wait_recv()
    low_w = split(template_filters(low_r, low_all, count_ref[2]))
    parts_low = []
    for c in range(low_chunks):
        at = (low_chunks - 1 - c) * LANES
        parts_low.append(dot3(low_w, (fl_top[at : at + LANES, :LANES], fl_rest[at : at + LANES, :LANES])))
    low = jnp.concatenate(parts_low, axis=1)
    time = y * low_here - (HALF_TAPS + 1) + lax.broadcasted_iota(jnp.int32, low.shape, 1)
    low = split(jnp.where((time >= 0) & (time < low_total), low, 0.0))
    for copy in landed[0]:
        copy.wait_recv()
    mid_w = split(template_filters(mid_r, mid_all, count_ref[1]))
    last_pieces(*(1, high_all))
    width, columns = g_top.shape[1], p_top.shape[1]
    for start in range(0, columns, WIDE):
        size_here = min(WIDE, columns - start)
        at = (mid_chunks - taps_mid // LANES - start // LANES) * LANES
        frames = (fm_top[at : at + taps_mid, :size_here], fm_rest[at : at + taps_mid, :size_here])
        value = dot3(mid_w, frames)
        base_col, lead = start // width * LANES, start % width
        tile = slice(lead, lead + size_here)
        pieces = tuple(v[:, base_col : base_col + WIDE] for v in low)
        value += dot3(pieces, (g_top[:, tile], g_rest[:, tile]))
        time = y * mid_here - HALF_TAPS + start + lax.broadcasted_iota(jnp.int32, value.shape, 1)
        top, rest = split(jnp.where((time >= 0) & (time < mid_total), value, 0.0))
        p_top[:, start : start + size_here] = top
        p_rest[:, start : start + size_here] = rest
    for copy in landed[1]:
        copy.wait_recv()
    w_top[...], w_rest[...] = split(template_filters(high_r, high_all, count_ref[0]))
    for copy in sent:
        copy.wait_send()
    for copy in stores:
        copy.wait()


def bounds(s_low, s_mid, slices):
    low, mid = s_low.shape[0] * LANES, s_mid.shape[0] * LANES
    return low, mid, low * slices, mid * slices


def template_filters(recon_ref, full, count):
    peers, rows, taps = full.shape
    first = (((0,), (0,)), ((), ()))
    index = lax.broadcasted_iota(jnp.int32, recon_ref.shape, 0)
    recon = jnp.where(index < count, recon_ref[...], 0.0)
    if rows % 8 == 0:
        return dot3(split(recon), split(full[...].reshape(peers * rows, taps)), first)
    total = 0.0
    for p in range(peers):
        total += dot3(split(recon[p * rows : (p + 1) * rows]), split(full[p]), first)
    return total


def gather(sizes, count, filters, strains, g, recons):
    low, mid, high = filters
    s_low, s_mid, s_high = strains
    bands, peers, slices = sizes
    lines = 2 if peers % 2 == 0 else 1
    rings = peers // lines
    parts = math.gcd(slices, min(mid.shape[1], high.shape[1]) // (bands * LANES))
    f32, half = jnp.float32, jnp.bfloat16
    basis, _, tmpl = recons[0].shape
    taps_low, taps_mid, taps = (f.shape[1] for f in filters)
    low_here, mid_here, _, _ = bounds(s_low, s_mid, slices)
    samples = s_high.shape[0] * LANES
    columns = mid_here + LANES
    vmem = pl.BlockSpec(memory_space=pltpu.VMEM)
    anywhere = pl.BlockSpec(memory_space=pl.ANY)
    dma = pltpu.SemaphoreType.DMA

    def two(*dims):
        return [dma(dims)] * 2

    def frames(rows):
        return [pltpu.VMEM((rows, WIDE), half)] * 2

    return pl.pallas_call(
        functools.partial(gather_kernel, (bands, peers, slices, lines, parts)),
        out_shape=[jax.ShapeDtypeStruct((tmpl, taps), half)] * 2
        + [jax.ShapeDtypeStruct((tmpl, columns), half)] * 2
        + [jax.ShapeDtypeStruct((samples + taps, WIDE), half)] * 2,
        in_specs=[pl.BlockSpec(memory_space=pltpu.SMEM)] + [vmem] * 8 + [anywhere] * 3,
        out_specs=[vmem] * 4 + [anywhere] * 2,
        scratch_shapes=[pltpu.VMEM((peers,) + a.shape, f32) for a in filters]
        + [pltpu.VMEM((slices + 4,) + a.shape, f32) for a in (s_low, s_mid)]
        + [pltpu.VMEM((taps // LANES, LANES), f32)]
        + [pltpu.VMEM((basis, tmpl), f32)] * 3
        + [dma((3,)), dma((3, 2)), pltpu.VMEM(((samples + taps) // LANES, LANES), f32)]
        + frames(low_here + 2 * LANES + taps_low) + frames(columns + taps_mid) + frames(samples + taps)
        + two(3, slices) + two(rings) + two(rings) + two(2, rings)
        + two(2, parts, rings) * 3 + two(2, peers * parts),
        compiler_params=pltpu.CompilerParams(
            collective_id=0, has_side_effects=True, vmem_limit_bytes=60 * 1024 * 1024
        ),
        name="gather_filters",
    )(count, *filters, *strains, *g, *recons)


def split(value):
    top = value.astype(jnp.bfloat16)
    return top, (value - top.astype(jnp.float32)).astype(jnp.bfloat16)


def dot3(a, b, dims=(((1,), (0,)), ((), ()))):
    def one(u, v):
        return lax.dot_general(u, v, dims, preferred_element_type=jnp.float32)

    return one(a[0], b[0]) + one(a[0], b[1]) + one(a[1], b[0])


def staggered(row):
    return pltpu.roll(jnp.broadcast_to(row, (LANES, LANES)), 0, 1, stride=1, stride_axis=0)


def shifted(read, by):
    lane = lax.broadcasted_iota(jnp.int32, (1, LANES), 1)

    def row(r):
        late = [pltpu.roll(read(r + i), by, 1) for i in range(2)]
        return jnp.where(lane >= by, late[1], late[0])

    return row


def fill_frames(row, top_ref, rest_ref, chunks, first=0, last=None):
    lane = lax.broadcasted_iota(jnp.int32, (LANES, LANES), 1)
    lag = lax.broadcasted_iota(jnp.int32, (LANES, LANES), 0)

    def step(c, before):
        now = staggered(row(c + 1))
        top, rest = split(jnp.where(lane >= lag, now, before))
        left = pl.multiple_of((chunks - 1 - c) * LANES, LANES)
        right = pl.multiple_of((chunks - c) * LANES, LANES)
        for ref, value in ((top_ref, top), (rest_ref, rest)):
            ref[pl.ds(left, LANES), :LANES] = value
            ref[pl.ds(right, LANES), LANES:] = value
        return now

    lax.fori_loop(first, chunks if last is None else last, step, staggered(row(first)))


def compute_kernel(
    w_top, w_rest, p_top, p_rest, g_top, g_rest, frames_top, frames_rest,
    out_ref, fh_top, fh_rest, frame_sem,
):
    step = pl.program_id(0)
    blocks = pl.num_programs(0)
    taps = w_top.shape[1]
    width = out_ref.shape[2]
    chunks = fh_top.shape[0] // LANES - 1

    def block(j):
        rows = pl.ds(pl.multiple_of(j * width, width), width)
        return [
            pltpu.make_async_copy(src.at[rows], dst.at[rows], frame_sem.at[j, i])
            for i, (src, dst) in enumerate(((frames_top, fh_top), (frames_rest, fh_rest)))
        ]

    total = fh_top.shape[0] // width
    ahead = taps // width

    @pl.when(step == 0)
    def _():
        for j in reversed(range(total)):
            for copy in block(j):
                copy.start()
        for j in range(total - ahead, total):
            for copy in block(j):
                copy.wait()

    for copy in block(blocks - 1 - step):
        copy.wait()
    base = pl.multiple_of(step * (width // RATIO), LANES)
    pieces = (p_top[:, pl.ds(base, WIDE)], p_rest[:, pl.ds(base, WIDE)])
    near = [piece[:, :LANES] for piece in pieces]
    stacked = jnp.concatenate(near, axis=1)
    for start in range(0, width, WIDE):
        at = (chunks - taps // LANES - start // LANES - step * (width // LANES)) * LANES
        rows = pl.ds(pl.multiple_of(at, LANES), taps)
        value = dot3((w_top[...], w_rest[...]), (fh_top[rows, :], fh_rest[rows, :]))
        tile = slice(start, start + WIDE)
        if (start + WIDE) // RATIO + 2 * HALF_TAPS <= LANES:
            top = g_top[:LANES, tile]
            value += jnp.dot(
                stacked, jnp.concatenate([top, top], axis=0), preferred_element_type=jnp.float32
            )
            value += jnp.dot(near[0], g_rest[:LANES, tile], preferred_element_type=jnp.float32)
        else:
            value += dot3(pieces, (g_top[:, tile], g_rest[:, tile]))
        out_ref[0, :, tile] = value


def compute(w, p, g, frames):
    tmpl, taps = w[0].shape
    rows = frames[0].shape[0]
    samples = rows - taps
    width = g[0].shape[1]
    vmem = pl.BlockSpec(memory_space=pltpu.VMEM)
    return pl.pallas_call(
        compute_kernel,
        grid=(samples // width,),
        out_shape=jax.ShapeDtypeStruct((1, tmpl, samples), jnp.float32),
        in_specs=[vmem] * 6 + [pl.BlockSpec(memory_space=pl.ANY)] * 2,
        out_specs=pl.BlockSpec((1, tmpl, width), lambda i: (0, 0, i)),
        scratch_shapes=[pltpu.VMEM((rows, WIDE), jnp.bfloat16)] * 2
        + [pltpu.SemaphoreType.DMA((rows // width, 2))],
        compiler_params=pltpu.CompilerParams(vmem_limit_bytes=60 * 1024 * 1024),
        name="filter_templates",
    )(*w, *p, *g, *frames)


def local(
    sizes, strain_high, strain_mid, strain_low, filters_high, filters_mid, filters_low,
    recon_high, recon_mid, recon_low, basis_count,
):
    matrix = upsample_matrix(WIDE, RATIO * LANES)
    top = matrix.astype(jnp.bfloat16)
    rest = (matrix - top.astype(np.float32)).astype(jnp.bfloat16)
    g = (jnp.asarray(top), jnp.asarray(rest))
    strains = [s.reshape(-1, LANES) for s in (strain_low, strain_mid, strain_high)]
    out = gather(
        sizes, basis_count, (filters_low, filters_mid, filters_high), strains, g,
        (recon_low, recon_mid, recon_high),
    )
    return compute(out[:2], out[2:4], g, out[4:])


def solution(mesh):
    sizes = tuple(mesh.shape[name] for name in ("band", "tmpl", "tm"))
    in_specs = (
        P("tm"), P("tm"), P("tm"),
        P("tmpl", None), P("tmpl", None), P("tmpl", None),
        P(None, None, "tmpl"), P(None, None, "tmpl"), P(None, None, "tmpl"),
        P(),
    )
    return jax.shard_map(
        functools.partial(local, sizes), mesh=mesh, in_specs=in_specs,
        out_specs=P("band", "tmpl", "tm"), check_vma=False,
    )
```
